32 devices in a mesh: row: 4 (over y, core), col: 8 (over z, x).
Axes of the slice: x: 2, y: 2, z: 4, core: 2. Of those that a mesh axis runs over, the one named last changes fastest.
Arguments:
- demand: bfloat16 [12288, 128], P(('row', 'col')), may hold values from -6 to 6
- tile_data: bfloat16 [4, 8, 128, 128, 128], P('row', 'col'), may hold values from -0.078125 to 0.078125
- tile_row: int32 [4, 8, 128], P('row', 'col'), may hold values from 0 to 12, as said below
- tile_col: int32 [4, 8, 128], P('row', 'col'), may hold values from 0 to 23, as said below
Outputs:
- leontief: bfloat16 [12288, 128], P(('row', 'col'))
The draws below stay inside these ranges and needn't reach their ends.
Inputs may be any that keep to these rules, and one draw needn't show every extreme that they name: `tile_row`: the value 4 * 3 marks an empty slot. In every index pair the live slots come first and number at least 42; in every draw some index pair has all 128 slots live. Two slots may name the same tile position; their tiles then add. `tile_col`: empty slots carry a column too, which is ignored.
All inputs are finite; a program needn't handle non-finite values.
Results may differ from the reference program's by a relative error of at most 0.018.
Values may be sent and summed in bfloat16 or wider, within the bound.
A program may use at most 64 MiB of HBM per device.

```python
import jax
import jax.numpy as jnp
from jax import lax

TILE = 128
SPAN = 3
COLS = 128
SLOTS = 128
SECTORS = 12288
N_ROW = 4
N_COL = 8


def draw_tile_row(key, part):
    key_count = jax.random.fold_in(key, 11)
    key_full = jax.random.fold_in(key, 12)
    key_rows = jax.random.fold_in(key, 13)
    counts = jax.random.randint(key_count, (N_ROW, N_COL), SLOTS // 3, SLOTS + 1)
    chosen = jax.random.randint(key_full, (), 0, N_ROW * N_COL)
    flat_index = jnp.arange(N_ROW * N_COL, dtype=jnp.int32).reshape(N_ROW, N_COL)
    counts = jnp.where(flat_index == chosen, SLOTS, counts)
    rows_drawn = jax.random.randint(key_rows, (N_ROW, N_COL, SLOTS), 0, N_ROW * SPAN)
    slot_index = jnp.arange(SLOTS, dtype=jnp.int32)
    live = slot_index[None, None, :] < counts[:, :, None]
    return jnp.where(live, rows_drawn, N_ROW * SPAN).astype(jnp.int32)


def draw_tile_col(key, part):
    key_cols = jax.random.fold_in(key, 21)
    return jax.random.randint(key_cols, (N_ROW, N_COL, SLOTS), 0, N_COL * SPAN).astype(jnp.int32)


def block_levels(stream_key, dims, pieces, least, largest):
    def one(position, blocks):
        steps = jax.random.uniform(jax.random.fold_in(jax.random.fold_in(stream_key, 6), position), (blocks,), jnp.float32, least / len(pieces), largest / len(pieces))
        return jnp.repeat(jnp.exp(steps), dims[position] // blocks).reshape((-1,) + (1,) * (len(dims) - position - 1))

    gain = one(*pieces[0])
    for cut in pieces[1:]:
        gain = gain * one(*cut)
    return gain


def noise(key, dims, deviation, bound, split=(), kind=jnp.bfloat16):
    drawn = deviation * jax.random.normal(key, dims, jnp.float32)
    if split:
        drawn = drawn * block_levels(key, dims, split, -0.22, 0.18)
    return jnp.clip(drawn, -bound, bound).astype(kind)


def setup_inputs(seed: int = 0) -> dict:
    key_of = jax.random.split(jax.random.key(seed), 5)
    demand = noise(key_of[0], (SECTORS, COLS), 1.0, 6.0, ((0, 32),))
    tile_data = noise(key_of[1], (N_ROW, N_COL, SLOTS, TILE, TILE), (SLOTS * TILE // SPAN) ** -0.5, 0.078125, ((0, 4), (1, 8)))
    tile_row = draw_tile_row(jax.random.fold_in(key_of[4], 71), 0)
    tile_col = draw_tile_col(jax.random.fold_in(key_of[4], 71), 0)
    return {"demand": demand, "tile_data": tile_data, "tile_row": tile_row, "tile_col": tile_col}


def multiply(panel, tile_data, tile_row, tile_col):
    columns = panel.shape[1]
    local_rows = N_ROW * SPAN
    blocks = panel.reshape(N_ROW, N_COL * SPAN, TILE, columns)
    targets = jnp.arange(local_rows, dtype=jnp.int32)

    def per_target(target):
        def accumulate(running, source):
            picked = jnp.take(blocks[source], tile_col[source, target], axis=0)
            products = jnp.einsum("stk,skc->stc", tile_data[source, target].astype(jnp.float32), picked.astype(jnp.float32))
            onehot = (tile_row[source, target][None, :] == targets[:, None]).astype(jnp.float32)
            partial_value = jnp.dot(onehot, products.reshape(SLOTS, -1), precision=lax.Precision.HIGHEST)
            partial_value = lax.optimization_barrier(partial_value.astype(jnp.bfloat16)).astype(jnp.float32)
            return running + partial_value, None

        running, _ = lax.scan(accumulate, jnp.zeros((local_rows, TILE * columns), jnp.float32), jnp.arange(N_ROW, dtype=jnp.int32))
        return running.astype(jnp.bfloat16).reshape(N_ROW, SPAN * TILE, columns)

    stacked = lax.map(per_target, jnp.arange(N_COL, dtype=jnp.int32))
    return stacked.transpose(1, 0, 2, 3).reshape(-1, columns)


def reference(demand, tile_data, tile_row, tile_col):
    first_term = multiply(demand, tile_data, tile_row, tile_col)
    second_term = multiply(first_term, tile_data, tile_row, tile_col)
    summed = demand.astype(jnp.float32) + first_term.astype(jnp.float32) + second_term.astype(jnp.float32)
    return summed.astype(jnp.bfloat16)
```

```python
import functools

import jax
import jax.numpy as jnp
from jax import lax
from jax.experimental import pallas as pl
from jax.experimental.pallas import tpu as pltpu
from jax.sharding import PartitionSpec as P

GROUP = 2
UNROLL = 10
MESH = pl.DeviceIdType.MESH


def schedule(slot_rows, slot_cols, local_rows, zero_block, units):
    slots = slot_rows.shape[0]
    index = jnp.arange(slots, dtype=jnp.int32)
    same = slot_rows[:, None] == slot_rows[None, :]
    earlier = index[None, :] < index[:, None]
    live = slot_rows < local_rows
    prior = jnp.sum((same & earlier).astype(jnp.int32), axis=1)
    opens = live & (prior % GROUP == 0)
    below = slot_rows[None, :] < slot_rows[:, None]
    base = jnp.sum((below & opens[None, :]).astype(jnp.int32), axis=1)
    place = jnp.where(live, base * GROUP + prior, -1)
    spots = jnp.arange(units * GROUP, dtype=jnp.int32)
    hit = place[None, :] == spots[:, None]
    source = jnp.sum(jnp.where(hit, index[None, :], 0), axis=1)
    column = zero_block + jnp.sum(jnp.where(hit, slot_cols[None, :] - zero_block, 0), axis=1)
    heads = place[None, :] == jnp.arange(units, dtype=jnp.int32)[:, None] * GROUP
    keep = 1 - jnp.sum((heads & (prior == 0)[None, :]).astype(jnp.int32), axis=1)
    targets = jnp.arange(local_rows, dtype=jnp.int32)
    mine = slot_rows[None, :] == targets[:, None]
    last = jnp.max(jnp.where(mine, place[None, :] // GROUP, -1), axis=1)
    last = jnp.where(last < 0, units, last)
    return jnp.concatenate([source, column, keep, last])


def kernel(n_row, n_col, n_x, units, plan, demand, tile_hbm, out, tiles, panel_a, panel_b, products,
           packed, landed, first, tile_sem, sx, rx, su, ru, sd, rd, sh, rh, sr, rr):
    n_z = n_col // n_x
    span, edge, columns = demand.shape
    zero_block = n_col * span
    spots = units * GROUP
    half = span // 2 if n_x > 1 else 0
    row = lax.axis_index("row")
    col = lax.axis_index("col")
    z = col // n_x
    x = col % n_x
    peer = z * n_x + (n_x - 1 - x)
    up_ok = z < n_z - 1
    down_ok = z > 0

    tile_copy = pltpu.make_async_copy(tile_hbm.at[0, 0], tiles, tile_sem)
    tile_copy.start()

    barrier = pltpu.get_barrier_semaphore()

    def greet(r, c):
        pl.semaphore_signal(barrier, inc=1, device_id=(r, c), device_id_type=MESH)

    for step in range(1, n_row):
        greet((row + step) % n_row, col)
    if n_x > 1:
        greet(row, peer)
    pl.when(up_ok)(lambda: greet(row, col + n_x))
    pl.when(down_ok)(lambda: greet(row, col - n_x))

    for panel in (panel_a, panel_b):
        panel[zero_block] = jnp.zeros((edge, columns), panel.dtype)
    products[units] = jnp.zeros((edge, columns), jnp.float32)
    panel_a[pl.ds(col * span, span)] = demand[...]
    greeted = n_row - 1 + (1 if n_x > 1 else 0) + up_ok.astype(jnp.int32) + down_ok.astype(jnp.int32)
    pl.semaphore_wait(barrier, greeted)

    def remote(src, dst, send, recv, target):
        return pltpu.make_async_remote_copy(
            src_ref=src, dst_ref=dst, send_sem=send, recv_sem=recv, device_id=(row, target), device_id_type=MESH
        )

    def gather(turn, own, panel):
        def block(c, start=0, stop=span):
            return panel.at[pl.ds(c * span + start, stop - start)]

        def cross(c, offset, src=None, start=0):
            at = (turn, offset + n_z - 1)
            return remote(block(c, start) if src is None else src, block(c, start), sx.at[at], rx.at[at], peer)

        def upward(c, away, src=None):
            return remote(block(c) if src is None else src, block(c), su.at[turn, away], ru.at[turn, away + 1], col + n_x)

        def downward(c, away, src=None):
            return remote(block(c) if src is None else src, block(c), sd.at[turn, away], rd.at[turn, away + 1], col - n_x)

        def side(c, way, target):
            return remote(block(c, 0, half), block(c, 0, half), sh.at[turn, way], rh.at[turn, way], target)

        pl.when(up_ok)(lambda: upward(col, 0, own).start())
        pl.when(down_ok)(lambda: downward(col, 0, own).start())
        if n_x > 1:
            cross(col, 0, own).start()
        if half:
            cross(peer, 0).wait_recv()
            pl.when(up_ok)(lambda: side(peer, 0, col + n_x).start())
            pl.when(down_ok)(lambda: side(peer, 1, col - n_x).start())
        for away in range(1, n_z):
            skip = half if away == 1 else 0

            @pl.when(z >= away)
            def _():
                c = col - away * n_x
                remote(block(c), block(c), su.at[turn, away - 1], ru.at[turn, away], col).wait_recv()
                if n_x > 1:
                    cross(c, -away, start=skip).start()
                if away + 1 < n_z:
                    pl.when(up_ok)(lambda: upward(c, away).start())

            @pl.when(z + away < n_z)
            def _():
                c = col + away * n_x
                remote(block(c), block(c), sd.at[turn, away - 1], rd.at[turn, away], col).wait_recv()
                if n_x > 1:
                    cross(c, away, start=skip).start()
                if away + 1 < n_z:
                    pl.when(down_ok)(lambda: downward(c, away).start())

        if n_x > 1:
            if half:
                pl.when(down_ok)(lambda: side(peer - n_x, 0, col).wait_recv())
                pl.when(up_ok)(lambda: side(peer + n_x, 1, col).wait_recv())
            else:
                cross(peer, 0).wait_recv()
            for away in range(1, n_z):
                skip = half if away == 1 else 0
                pl.when(z >= away)(lambda: cross(peer - away * n_x, -away, start=skip).wait_recv())
                pl.when(z + away < n_z)(lambda: cross(peer + away * n_x, away, start=skip).wait_recv())

        def drain():
            pl.when(up_ok)(lambda: upward(col, 0, own).wait_send())
            pl.when(down_ok)(lambda: downward(col, 0, own).wait_send())
            if n_x > 1:
                cross(col, 0, own).wait_send()
            if half:
                pl.when(up_ok)(lambda: side(peer, 0, col + n_x).wait_send())
                pl.when(down_ok)(lambda: side(peer, 1, col - n_x).wait_send())
            for away in range(1, n_z):
                skip = half if away == 1 else 0

                @pl.when(z >= away)
                def _():
                    c = col - away * n_x
                    if n_x > 1:
                        cross(c, -away, start=skip).wait_send()
                    if away + 1 < n_z:
                        pl.when(up_ok)(lambda: upward(c, away).wait_send())

                @pl.when(z + away < n_z)
                def _():
                    c = col + away * n_x
                    if n_x > 1:
                        cross(c, away, start=skip).wait_send()
                    if away + 1 < n_z:
                        pl.when(down_ok)(lambda: downward(c, away).wait_send())

        return drain

    def compute(panel):
        def body(step, total):
            for part in range(UNROLL):
                unit = step * UNROLL + part
                left = [tiles[plan[unit * GROUP + k]] for k in range(GROUP)]
                right = [panel[plan[spots + unit * GROUP + k]] for k in range(GROUP)]
                keep = plan[2 * spots + unit].astype(jnp.float32)
                total = total * keep + jnp.dot(
                    jnp.concatenate(left, axis=1), jnp.concatenate(right, axis=0), preferred_element_type=jnp.float32
                )
                products[unit] = total
            return total

        lax.fori_loop(0, units // UNROLL, body, jnp.zeros((edge, columns), jnp.float32))

    def scatter(turn):
        def pack(r):
            for k in range(span):
                packed[turn, r * span + k] = products[plan[2 * spots + units + r * span + k]].astype(packed.dtype)

        def send(step):
            r = (row + step) % n_row
            return pltpu.make_async_remote_copy(
                src_ref=packed.at[turn, pl.ds(r * span, span)],
                dst_ref=landed.at[turn, step - 1],
                send_sem=sr.at[turn, step - 1],
                recv_sem=rr.at[turn, step - 1],
                device_id=(r, col),
                device_id_type=MESH,
            )

        steps = sorted(range(1, n_row), key=lambda step: abs(step - n_row // 2))
        for step in steps:
            pack((row + step) % n_row)
            send(step).start()
        pack(row)
        value = packed[turn, pl.ds(row * span, span)].astype(jnp.float32)
        for step in range(1, n_row):
            send(step).wait_recv()
            value = value + landed[turn, step - 1].astype(jnp.float32)

        def drain():
            for step in range(1, n_row):
                send(step).wait_send()

        return value.astype(first.dtype), drain

    drains = [gather(0, demand, panel_a)]
    tile_copy.wait()
    compute(panel_a)
    value, drain = scatter(0)
    drains.append(drain)
    first[...] = value
    panel_b[pl.ds(col * span, span)] = value
    drains.append(gather(1, first, panel_b))
    compute(panel_b)
    value, drain = scatter(1)
    drains.append(drain)
    out[...] = (
        demand[...].astype(jnp.float32) + first[...].astype(jnp.float32) + value.astype(jnp.float32)
    ).astype(out.dtype)
    for drain in drains:
        drain()


def body(n_row, n_col, demand, tile_data, tile_row, tile_col):
    slots, edge = tile_data.shape[2], tile_data.shape[-1]
    columns = demand.shape[1]
    span = demand.shape[0] // edge
    local_rows = n_row * span
    n_x = 2 if n_col % 2 == 0 else 1
    n_z = n_col // n_x
    units = (slots + local_rows * (GROUP - 1)) // GROUP
    units = -(-units // UNROLL) * UNROLL
    plan = schedule(tile_row[0, 0], tile_col[0, 0], local_rows, n_col * span, units)
    dma = pltpu.SemaphoreType.DMA
    vmem = pl.BlockSpec(memory_space=pltpu.VMEM)
    result = pl.pallas_call(
        functools.partial(kernel, n_row, n_col, n_x, units),
        out_shape=jax.ShapeDtypeStruct((span, edge, columns), demand.dtype),
        in_specs=[pl.BlockSpec(memory_space=pltpu.SMEM), vmem, pl.BlockSpec(memory_space=pl.ANY)],
        out_specs=vmem,
        scratch_shapes=[
            pltpu.VMEM((slots, edge, edge), tile_data.dtype),
            pltpu.VMEM((n_col * span + 1, edge, columns), demand.dtype),
            pltpu.VMEM((n_col * span + 1, edge, columns), demand.dtype),
            pltpu.VMEM((units + 1, edge, columns), jnp.float32),
            pltpu.VMEM((2, local_rows, edge, columns), demand.dtype),
            pltpu.VMEM((2, n_row - 1, span, edge, columns), demand.dtype),
            pltpu.VMEM((span, edge, columns), demand.dtype),
            dma,
            dma((2, 2 * n_z - 1)),
            dma((2, 2 * n_z - 1)),
            dma((2, n_z + 1)),
            dma((2, n_z + 1)),
            dma((2, n_z + 1)),
            dma((2, n_z + 1)),
            dma((2, 2)),
            dma((2, 2)),
            dma((2, n_row - 1)),
            dma((2, n_row - 1)),
        ],
        compiler_params=pltpu.CompilerParams(
            collective_id=0, has_side_effects=True, vmem_limit_bytes=56 * 1024 * 1024
        ),
    )(plan, demand.reshape(span, edge, columns), tile_data)
    return result.reshape(demand.shape)


def solution(mesh):
    placed = (
        P(("row", "col"), None),
        P("row", "col", None, None, None),
        P("row", "col", None),
        P("row", "col", None),
    )
    return jax.shard_map(
        functools.partial(body, mesh.shape["row"], mesh.shape["col"]),
        mesh=mesh, in_specs=placed, out_specs=P(("row", "col"), None), check_vma=False,
    )
```

```python
import functools

import jax
import jax.numpy as jnp
from jax import lax
from jax.experimental import pallas as pl
from jax.experimental.pallas import tpu as pltpu
from jax.sharding import PartitionSpec as P

GROUP = 2
UNROLL = 10
CUTS = 1
MESH = pl.DeviceIdType.MESH


def schedule(rows_ref, cols_ref, plan_vector, local_rows, zero_block, units):
    slots = rows_ref.shape[1]
    width = plan_vector.shape[1]
    square = (slots, slots)
    row_lane = jnp.broadcast_to(rows_ref[...], square)
    row_sub = jnp.transpose(row_lane)
    col_sub = jnp.transpose(jnp.broadcast_to(cols_ref[...], square))[:, 0:1]
    lane = lax.broadcasted_iota(jnp.int32, square, 1)
    sub = lax.broadcasted_iota(jnp.int32, square, 0)
    same = row_lane == row_sub
    prior_sub = jnp.sum(jnp.where(same & (lane < sub), 1, 0), axis=1, keepdims=True)
    prior_lane = jnp.sum(jnp.where(same & (sub < lane), 1, 0), axis=0, keepdims=True)
    opens = jnp.where((prior_lane & (GROUP - 1)) == 0, 1, 0)
    base = jnp.sum(jnp.where(row_lane < row_sub, jnp.broadcast_to(opens, square), 0), axis=1, keepdims=True)
    mine = row_sub[:, 0:1]
    place = jnp.where(mine < local_rows, base * GROUP + prior_sub, -1)
    wide = (slots, width)
    spot = lax.broadcasted_iota(jnp.int32, wide, 1)
    hit = jnp.broadcast_to(place, wide) == spot
    slot = lax.broadcasted_iota(jnp.int32, wide, 0)

    def total(value):
        return jnp.sum(jnp.where(hit, value, 0), axis=0, keepdims=True)

    plan_vector[0:1, :] = total(slot)
    plan_vector[1:2, :] = zero_block + total(jnp.broadcast_to(col_sub - zero_block, wide))
    plan_vector[2:3, :] = 1 - total(jnp.broadcast_to(jnp.where(prior_sub == 0, 1, 0), wide))
    here = jnp.broadcast_to(mine, wide) == spot
    unit = jnp.broadcast_to(lax.shift_right_arithmetic(place, GROUP // 2), wide)
    last = jnp.max(jnp.where(here, unit, -1), axis=0, keepdims=True)
    plan_vector[3:4, :] = jnp.where(last < 0, units, last)


def kernel(n_row, n_col, n_x, units, rows_ref, cols_ref, demand, tile_hbm, out, tiles, panel_a, panel_b, products,
           packed, landed, first, plan_vector, plan, tile_sem, plan_sem, sx, rx, su, ru, sd, rd, sr, rr):
    n_z = n_col // n_x
    span, edge, columns = demand.shape
    zero_block = n_col * span
    depth = edge // CUTS
    pieces = span * CUTS
    row = lax.axis_index("row")
    col = lax.axis_index("col")
    z = col // n_x
    x = col % n_x
    peer = z * n_x + (n_x - 1 - x)
    up_ok = z < n_z - 1
    down_ok = z > 0

    tile_copy = pltpu.make_async_copy(tile_hbm.at[0, 0], tiles, tile_sem)
    tile_copy.start()

    barrier = pltpu.get_barrier_semaphore()

    def greet(r, c):
        pl.semaphore_signal(barrier, inc=1, device_id=(r, c), device_id_type=MESH)

    for step in range(1, n_row):
        greet((row + step) % n_row, col)
    if n_x > 1:
        greet(row, peer)
    pl.when(up_ok)(lambda: greet(row, col + n_x))
    pl.when(down_ok)(lambda: greet(row, col - n_x))

    for panel in (panel_a, panel_b):
        panel[zero_block] = jnp.zeros((edge, columns), panel.dtype)
    products[units] = jnp.zeros((edge, columns), jnp.float32)
    panel_a[pl.ds(col * span, span)] = demand[...]
    greeted = n_row - 1 + (1 if n_x > 1 else 0) + up_ok.astype(jnp.int32) + down_ok.astype(jnp.int32)
    pl.semaphore_wait(barrier, greeted)

    def remote(src, dst, send, recv, target):
        return pltpu.make_async_remote_copy(
            src_ref=src, dst_ref=dst, send_sem=send, recv_sem=recv, device_id=(row, target), device_id_type=MESH
        )

    def gather(turn, own, panel, ready):
        def piece(ref, tile, p):
            return ref.at[tile + p // CUTS, pl.ds((p % CUTS) * depth, depth)]

        def cross(c, offset, p, src=None):
            at = (turn, offset + n_z - 1, p)
            there = piece(panel, c * span, p)
            return remote(there if src is None else piece(src, 0, p), there, sx.at[at], rx.at[at], peer)

        def upward(c, away, p, src=None):
            there = piece(panel, c * span, p)
            here = there if src is None else piece(src, 0, p)
            return remote(here, there, su.at[turn, away, p], ru.at[turn, away + 1, p], col + n_x)

        def downward(c, away, p, src=None):
            there = piece(panel, c * span, p)
            here = there if src is None else piece(src, 0, p)
            return remote(here, there, sd.at[turn, away, p], rd.at[turn, away + 1, p], col - n_x)

        def arrived(c, sem, away, p):
            there = piece(panel, c * span, p)
            remote(there, there, sem.at[turn, away, p], sem.at[turn, away, p], peer).wait_recv()

        for p in range(pieces):
            if p % CUTS == 0:
                ready(p // CUTS)
            pl.when(up_ok)(lambda: upward(col, 0, p, own).start())
            pl.when(down_ok)(lambda: downward(col, 0, p, own).start())
            if n_x > 1:
                cross(col, 0, p, own).start()
        ready(span)
        for away in range(1, n_z):
            for p in range(pieces):

                @pl.when(z >= away)
                def _():
                    c = col - away * n_x
                    arrived(c, ru, away, p)
                    if away + 1 < n_z:
                        pl.when(up_ok)(lambda: upward(c, away, p).start())
                    if n_x > 1:
                        cross(c, -away, p).start()

                @pl.when(z + away < n_z)
                def _():
                    c = col + away * n_x
                    arrived(c, rd, away, p)
                    if away + 1 < n_z:
                        pl.when(down_ok)(lambda: downward(c, away, p).start())
                    if n_x > 1:
                        cross(c, away, p).start()

        if n_x > 1:
            for p in range(pieces):
                cross(peer, 0, p).wait_recv()
                for away in range(1, n_z):
                    pl.when(z >= away)(lambda: cross(peer - away * n_x, -away, p).wait_recv())
                    pl.when(z + away < n_z)(lambda: cross(peer + away * n_x, away, p).wait_recv())

        def drain():
            for p in range(pieces):
                pl.when(up_ok)(lambda: upward(col, 0, p, own).wait_send())
                pl.when(down_ok)(lambda: downward(col, 0, p, own).wait_send())
                if n_x > 1:
                    cross(col, 0, p, own).wait_send()
                for away in range(1, n_z):

                    @pl.when(z >= away)
                    def _():
                        c = col - away * n_x
                        if n_x > 1:
                            cross(c, -away, p).wait_send()
                        if away + 1 < n_z:
                            pl.when(up_ok)(lambda: upward(c, away, p).wait_send())

                    @pl.when(z + away < n_z)
                    def _():
                        c = col + away * n_x
                        if n_x > 1:
                            cross(c, away, p).wait_send()
                        if away + 1 < n_z:
                            pl.when(down_ok)(lambda: downward(c, away, p).wait_send())

        return drain

    def compute(panel):
        def body(step, total):
            for part in range(UNROLL):
                unit = step * UNROLL + part
                left = [tiles[plan[0, unit * GROUP + k]] for k in range(GROUP)]
                right = [panel[plan[1, unit * GROUP + k]] for k in range(GROUP)]
                keep = plan[2, unit * GROUP].astype(jnp.float32)
                total = total * keep + jnp.dot(
                    jnp.concatenate(left, axis=1), jnp.concatenate(right, axis=0), preferred_element_type=jnp.float32
                )
                products[unit] = total
            return total

        lax.fori_loop(0, units // UNROLL, body, jnp.zeros((edge, columns), jnp.float32))

    def send(turn, step, k):
        r = (row + step) % n_row
        return pltpu.make_async_remote_copy(
            src_ref=packed.at[turn, r * span + k],
            dst_ref=landed.at[turn, step - 1, k],
            send_sem=sr.at[turn, step - 1, k],
            recv_sem=rr.at[turn, step - 1, k],
            device_id=(r, col),
            device_id_type=MESH,
        )

    def scatter(turn):
        steps = sorted(range(1, n_row), key=lambda step: abs(step - n_row // 2))
        for k in range(span):
            for step in steps:
                r = (row + step) % n_row
                packed[turn, r * span + k] = products[plan[3, r * span + k]].astype(packed.dtype)
                send(turn, step, k).start()

        def drain():
            for k in range(span):
                for step in steps:
                    send(turn, step, k).wait_send()

        return drain

    def collect(turn, k):
        value = products[plan[3, row * span + k]]
        for step in range(1, n_row):
            send(turn, step, k).wait_recv()
            value = value + landed[turn, step - 1, k].astype(jnp.float32)
        return value.astype(first.dtype)

    def ready_a(k):
        if k == span:
            schedule(rows_ref, cols_ref, plan_vector, n_row * span, zero_block, units)
            plan_copy = pltpu.make_async_copy(plan_vector, plan, plan_sem)
            plan_copy.start()
            plan_copy.wait()

    def ready_b(k):
        if k < span:
            value = collect(0, k)
            first[k] = value
            panel_b[col * span + k] = value

    drains = [gather(0, demand, panel_a, ready_a)]
    tile_copy.wait()
    compute(panel_a)
    drains.append(scatter(0))
    drains.append(gather(1, first, panel_b, ready_b))
    compute(panel_b)
    drains.append(scatter(1))
    for k in range(span):
        value = collect(1, k)
        out[k] = (
            demand[k].astype(jnp.float32) + first[k].astype(jnp.float32) + value.astype(jnp.float32)
        ).astype(out.dtype)
    for drain in drains:
        drain()


def body(n_row, n_col, demand, tile_data, tile_row, tile_col):
    slots, edge = tile_data.shape[2], tile_data.shape[-1]
    columns = demand.shape[1]
    span = demand.shape[0] // edge
    local_rows = n_row * span
    n_x = 2 if n_col % 2 == 0 else 1
    n_z = n_col // n_x
    units = (slots + local_rows * (GROUP - 1)) // GROUP
    units = -(-units // UNROLL) * UNROLL
    width = -(-max(units * GROUP, local_rows) // 128) * 128
    pieces = span * CUTS
    dma = pltpu.SemaphoreType.DMA
    vmem = pl.BlockSpec(memory_space=pltpu.VMEM)
    result = pl.pallas_call(
        functools.partial(kernel, n_row, n_col, n_x, units),
        out_shape=jax.ShapeDtypeStruct((span, edge, columns), demand.dtype),
        in_specs=[vmem, vmem, vmem, pl.BlockSpec(memory_space=pl.ANY)],
        out_specs=vmem,
        scratch_shapes=[
            pltpu.VMEM((slots, edge, edge), tile_data.dtype),
            pltpu.VMEM((n_col * span + 1, edge, columns), demand.dtype),
            pltpu.VMEM((n_col * span + 1, edge, columns), demand.dtype),
            pltpu.VMEM((units + 1, edge, columns), jnp.float32),
            pltpu.VMEM((2, local_rows, edge, columns), demand.dtype),
            pltpu.VMEM((2, n_row - 1, span, edge, columns), demand.dtype),
            pltpu.VMEM((span, edge, columns), demand.dtype),
            pltpu.VMEM((8, width), jnp.int32),
            pltpu.SMEM((8, width), jnp.int32),
            dma,
            dma,
            dma((2, 2 * n_z - 1, pieces)),
            dma((2, 2 * n_z - 1, pieces)),
            dma((2, n_z + 1, pieces)),
            dma((2, n_z + 1, pieces)),
            dma((2, n_z + 1, pieces)),
            dma((2, n_z + 1, pieces)),
            dma((2, n_row - 1, span)),
            dma((2, n_row - 1, span)),
        ],
        compiler_params=pltpu.CompilerParams(
            collective_id=0, has_side_effects=True, vmem_limit_bytes=56 * 1024 * 1024
        ),
    )(tile_row[0], tile_col[0], demand.reshape(span, edge, columns), tile_data)
    return result.reshape(demand.shape)


def solution(mesh):
    placed = (
        P(("row", "col"), None),
        P("row", "col", None, None, None),
        P("row", "col", None),
        P("row", "col", None),
    )
    return jax.shard_map(
        functools.partial(body, mesh.shape["row"], mesh.shape["col"]),
        mesh=mesh, in_specs=placed, out_specs=P(("row", "col"), None), check_vma=False,
    )
```
